32 devices in a mesh: ctx: 8 (over z, x), head: 4 (over y, core).
Axes of the slice: x: 2, y: 2, z: 4, core: 2. Of those that a mesh axis runs over, the one named last changes fastest.
Arguments:
- queries: bfloat16 [4096, 4096], P('ctx', 'head'), may hold values from -6 to 6
- keys: bfloat16 [2, 4096, 4096], P(None, 'ctx', 'head'), may hold values from -6 to 6
- values: bfloat16 [2, 4096, 4096], P(None, 'ctx', 'head'), may hold values from -6 to 6
- betas: float32 [32, 2, 4096], P('head', None, 'ctx'), may hold values from 1.9 to 2
- gate: bfloat16 [4096, 4096], P('ctx', 'head'), may hold values from -6 to 6
- out_weight: bfloat16 [4096, 4096], P('head'), may hold values from -0.125 to 0.125
Outputs:
- mixed: bfloat16 [4096, 4096], P('ctx', 'head')
The draws below stay inside these ranges and needn't reach their ends.
All inputs are finite; a program needn't handle non-finite values.
Results may differ from the reference program's by a relative error of at most 0.02.
Values may be sent and summed in bfloat16 or wider, within the bound.
A program may use at most 128 MiB of HBM per device.

```python
import math
import jax
import jax.numpy as jnp
from jax import lax

D = 4096
HEADS = 32
HEAD_DIM = 128
SPAN = 64
TOKENS = 4096
N_HEAD = 4


def strengthened(values, own_key, source, target, parts, factor):
    owner, partner = [(jnp.arange(values.shape[dim]) // (values.shape[dim] // parts)).reshape([-1 if axis == dim else 1 for axis in range(values.ndim)]) for dim in (source, target)]
    chosen = jax.random.permutation(own_key, parts)[partner]
    strong = (owner == chosen) | (owner == (partner + parts // 2) % parts)
    return jnp.where(strong, factor * values, values)


def block_levels(key, shape, shards, low, largest):
    gain, own = 1.0, jax.random.fold_in(key, 6)
    for axis_at, blocks in shards:
        heights = jnp.exp(jax.random.uniform(jax.random.fold_in(own, axis_at), (blocks,), jnp.float32, low / len(shards), largest / len(shards)))
        gain = gain * jnp.repeat(heights, shape[axis_at] // blocks).reshape([-1 if axis == axis_at else 1 for axis in range(len(shape))])
    return gain


def scatter_about(key, extent, deviation, limit, shards=(), kind=jnp.bfloat16):
    loudness = block_levels(key, extent, shards, -0.22, 0.18) if shards else 1.0
    values = jax.random.normal(key, extent, jnp.float32) * deviation * loudness
    return jnp.minimum(jnp.maximum(values, -limit), limit).astype(kind)


def noise_with(key, shape, deviation, limit, cuts, heavy, kind=jnp.bfloat16):
    entries = deviation * jax.random.normal(key, shape, jnp.float32)
    if cuts:
        entries = entries * block_levels(key, shape, cuts, -0.22, 0.18)
    return jnp.clip(strengthened(entries, jax.random.fold_in(key, 3), *heavy), -limit, limit).astype(kind)


def setup_inputs(seed: int = 0) -> dict:
    key_list = jax.random.split(jax.random.key(seed), 7)
    return {
        "queries": scatter_about(key_list[0], (TOKENS, HEADS * HEAD_DIM), 1.0, 6.0, ((0, 8), (1, 4))),
        "keys": scatter_about(key_list[1], (2, TOKENS, HEADS * HEAD_DIM), 1.0, 6.0, ((1, 8), (2, 4))),
        "values": scatter_about(key_list[2], (2, TOKENS, HEADS * HEAD_DIM), 1.0, 6.0, ((1, 8), (2, 4))),
        "betas": jnp.clip(1.9 + 0.100000024 * jax.random.uniform(key_list[3], (HEADS, 2, TOKENS), jnp.float32) ** block_levels(key_list[3], (HEADS, 2, TOKENS), ((0, 4), (2, 8)), -0.2, 0.2), 1.9, 2.0),
        "gate": scatter_about(key_list[4], (TOKENS, HEADS * HEAD_DIM), 1.0, 6.0, ((0, 8), (1, 4))),
        "out_weight": noise_with(key_list[5], (HEADS * HEAD_DIM, D), (HEADS * HEAD_DIM) ** -0.5, 0.125, ((0, 4),), (0, 1, 4, 2.0)),
    }


def product(left, right_part):
    return jnp.matmul(left, right_part, precision=lax.Precision.HIGHEST)

def flipped(array):
    return jnp.swapaxes(array, -1, -2)

def unit_rows(array):
    array = array.astype(jnp.float32)
    return array * lax.rsqrt(lax.optimization_barrier(jnp.sum(array * array, axis=-1, keepdims=True)) + 1e-06)

def unit_lower_solve(system, right_side):
    order = system.shape[-1]
    width = math.gcd(16, order)
    eye_block = jnp.eye(width, dtype=jnp.float32)
    pieces = []
    for index in range(order // width):
        first = index * width
        rhs = right_side[..., first:first + width, :]
        if index > 0:
            rhs = rhs - product(system[..., first:first + width, :first], jnp.concatenate(pieces, axis=-2))
        lower = system[..., first:first + width, first:first + width] - eye_block
        inverse = eye_block - lower
        power = lower
        degree = 1
        while 2 * degree < width:
            power = product(power, power)
            inverse = product(inverse, eye_block + power)
            degree = 2 * degree
        pieces.append(product(inverse, rhs))
    return jnp.concatenate(pieces, axis=-2)

def block_factors(keys_c, values_c, betas_c, queries_c):
    sub_steps = keys_c.shape[-2]
    block_tokens = queries_c.shape[-2]
    head_size = keys_c.shape[-1]
    row_index = lax.broadcasted_iota(jnp.int32, (sub_steps, sub_steps), 0)
    col_index = lax.broadcasted_iota(jnp.int32, (sub_steps, sub_steps), 1)
    strict_lower = (col_index < row_index).astype(jnp.float32)
    system = jnp.eye(sub_steps, dtype=jnp.float32) + betas_c[..., :, None] * product(keys_c, flipped(keys_c)) * strict_lower
    right_side = betas_c[..., :, None] * jnp.concatenate([keys_c, values_c], axis=-1)
    solved = unit_lower_solve(system, right_side)
    mixing = solved[..., :head_size]
    updates = solved[..., head_size:]
    query_row = lax.broadcasted_iota(jnp.int32, (block_tokens, sub_steps), 0)
    key_col = lax.broadcasted_iota(jnp.int32, (block_tokens, sub_steps), 1)
    causal = (key_col <= 2 * query_row + 1).astype(jnp.float32)
    scores = product(queries_c, flipped(keys_c)) * causal
    local_out = product(scores, updates)
    carry_map = queries_c - product(scores, mixing)
    transit = jnp.eye(head_size, dtype=jnp.float32) - product(flipped(keys_c), mixing)
    source = product(flipped(keys_c), updates)
    return (local_out, carry_map, transit, source)

def reference(queries, keys, values, betas, gate, out_weight):
    blocks = TOKENS // SPAN
    query_seq = queries.reshape(blocks, SPAN, HEADS, HEAD_DIM).transpose(0, 2, 1, 3)
    key_seq = keys.reshape(2, blocks, SPAN, HEADS, HEAD_DIM).transpose(1, 3, 2, 0, 4).reshape(blocks, HEADS, 2 * SPAN, HEAD_DIM)
    value_seq = values.reshape(2, blocks, SPAN, HEADS, HEAD_DIM).transpose(1, 3, 2, 0, 4).reshape(blocks, HEADS, 2 * SPAN, HEAD_DIM)
    beta_seq = betas.reshape(HEADS, 2, blocks, SPAN).transpose(2, 0, 3, 1).reshape(blocks, HEADS, 2 * SPAN)

    def advance(state, pieces):
        query_c, key_c, value_c, beta_c = pieces
        local_out, carry_map, transit, source = block_factors(unit_rows(key_c), value_c.astype(jnp.float32), beta_c, unit_rows(query_c))
        return (product(transit, state) + source, local_out + product(carry_map, state))
    start = jnp.zeros((HEADS, HEAD_DIM, HEAD_DIM), jnp.float32)
    final_state, outputs = lax.scan(advance, start, (query_seq, key_seq, value_seq, beta_seq))
    attended = outputs.transpose(0, 2, 1, 3).reshape(TOKENS, HEADS, HEAD_DIM)
    scale = lax.rsqrt(lax.optimization_barrier(jnp.mean(attended * attended, axis=-1, keepdims=True)) + 1e-06)
    mixed_in = (attended * scale * jax.nn.silu(gate.astype(jnp.float32).reshape(TOKENS, HEADS, HEAD_DIM))).astype(jnp.bfloat16)
    mixed_in = mixed_in.reshape(TOKENS, HEADS * HEAD_DIM)
    group = HEADS * HEAD_DIM // N_HEAD

    def add_group(index, total):
        cols = lax.dynamic_slice_in_dim(mixed_in, index * group, group, 1)
        weight = lax.dynamic_slice_in_dim(out_weight, index * group, group, 0)
        part_sum = jnp.dot(cols, weight, preferred_element_type=jnp.float32).astype(jnp.bfloat16)
        part_sum = lax.optimization_barrier(part_sum)
        return total + part_sum.astype(jnp.float32)
    total = lax.fori_loop(0, N_HEAD, add_group, jnp.zeros((TOKENS, D), jnp.float32))
    return total.astype(jnp.bfloat16)
```

```python
import functools

import jax
import jax.numpy as jnp
from jax import lax
from jax.experimental import pallas as pl
from jax.experimental.pallas import tpu as pltpu
from jax.sharding import PartitionSpec as P

HEAD_DIM = 128
SPAN = 64
BASE = 16
F32 = jnp.float32
BF16 = jnp.bfloat16
VMEM_LIMIT = 60 * 1024 * 1024


def iota(shape, dim):
    return lax.broadcasted_iota(jnp.int32, shape, dim)


def split(a):
    high = a.astype(BF16)
    return high, (a - high.astype(F32)).astype(BF16)


def dot(a, b):
    return jnp.dot(a, b, preferred_element_type=F32)


def dot3(a, b):
    ah, al = split(a)
    bh, bl = split(b)
    return dot(jnp.concatenate([ah, al, ah], axis=1), jnp.concatenate([bh, bh, bl], axis=0))


def inverse(lowers, order):
    lane = iota((BASE, order), 1)
    compact = []
    for low in lowers:
        total = jnp.zeros((BASE, order), F32)
        for blk in range(order // BASE):
            total = jnp.where(lane // BASE == blk, low[blk * BASE : (blk + 1) * BASE, :], total)
        compact.append(total)
    inv = [(iota((BASE, order), 0) == lane % BASE).astype(F32) for _ in lowers]
    for j in range(BASE - 1):
        pick = (lane // BASE) * BASE + j
        for n, low in enumerate(compact):
            column = jnp.take_along_axis(low, pick, axis=1, mode="promise_in_bounds")
            inv[n] = inv[n] - column * inv[n][j : j + 1, :]
    row = iota((order, order), 0)
    col = iota((order, order), 1)
    width = BASE
    while width < order:
        corner = (row // (2 * width) == col // (2 * width)) & (row // width != col // width)
        diagonal = row // width == col // width
        second = (iota((width, order), 1) // width) % 2 == 1
        half = [dot3(jnp.where(second, t, 0.0), jnp.where(corner, low, 0.0)) for t, low in zip(inv, lowers)]
        full = [
            jnp.where(diagonal, jnp.concatenate([t] * (order // width), axis=0), 0.0) for t in inv
        ]
        fill = [dot3(y, e) for y, e in zip(half, full)]
        inv = [
            jnp.concatenate([jnp.where(second, 0.0, t), jnp.where(second, t, 0.0) - r], axis=0)
            for t, r in zip(inv, fill)
        ]
        width *= 2
    return inv


def mix_kernel(q_ref, k_ref, v_ref, b_ref, o_ref, m_ref, x_out, x_ref):
    heads = q_ref.shape[1] // HEAD_DIM
    span = q_ref.shape[0]
    order = 2 * span
    step = pl.program_id(0)

    @pl.when(step == 0)
    def _():
        start = (iota((HEAD_DIM, 2 * HEAD_DIM), 0) == iota((HEAD_DIM, 2 * HEAD_DIM), 1)).astype(F32)
        for h in range(heads):
            x_ref[h] = start

    row = iota((order, order), 0)
    col = iota((order, order), 1)
    strict = col < row
    weave = (row == 2 * (col % span) + col // span).astype(BF16)
    causal = iota((span, order), 1) <= 2 * iota((span, order), 0) + 1
    data = []
    lowers = []
    for h in range(heads):
        cols = slice(h * HEAD_DIM, (h + 1) * HEAD_DIM)
        query = q_ref[:, cols]
        pair = jnp.concatenate(
            [
                jnp.concatenate([k_ref[0, :, cols], v_ref[0, :, cols]], axis=1),
                jnp.concatenate([k_ref[1, :, cols], v_ref[1, :, cols]], axis=1),
            ],
            axis=0,
        )
        woven = dot(weave, pair)
        key = woven[:, :HEAD_DIM]
        value = woven[:, HEAD_DIM:]
        key_b = key.astype(BF16)
        norm = lax.rsqrt(jnp.sum(key * key, axis=1, keepdims=True) + 1e-06)
        beta = b_ref[:, h : h + 1]
        both = jnp.concatenate([key_b, query], axis=0)
        gram = lax.dot_general(both, key_b, (((1,), (1,)), ((), ())), preferred_element_type=F32)
        weight = beta * norm * norm
        lowers.append(jnp.where(strict, weight * gram[:order], 0.0))
        scores = jnp.where(causal, gram[order:], 0.0).astype(BF16)
        qf = query.astype(F32)
        q_norm = lax.rsqrt(jnp.sum(qf * qf, axis=1, keepdims=True) + 1e-06)
        readers = jnp.concatenate([key.T.astype(BF16), scores], axis=0)
        data.append((both, readers, beta * norm * value, weight, q_norm))
    solved = inverse(lowers, order)
    seen = []
    for h in range(heads):
        both = data[h][0]
        high, low = split(x_ref[h])
        seen.append(
            dot(jnp.concatenate([both, both], axis=1), jnp.concatenate([high, low], axis=0))
        )
    writes = []
    for h in range(heads):
        _, _, scaled, weight, _ = data[h]
        gap = -weight * seen[h][:order]
        gap = jnp.concatenate([gap[:, :HEAD_DIM], gap[:, HEAD_DIM:] + scaled], axis=1)
        writes.append(dot3(solved[h], gap))
    for h in range(heads):
        cols = slice(h * HEAD_DIM, (h + 1) * HEAD_DIM)
        readers, q_norm = data[h][1], data[h][4]
        high, low = split(writes[h])
        change = dot(
            jnp.concatenate([readers, readers], axis=1), jnp.concatenate([high, low], axis=0)
        )
        x_ref[h] = x_ref[h] + change[:HEAD_DIM]
        out = q_norm * (seen[h][order:] + change[HEAD_DIM:])
        m_ref[:, cols] = out[:, :HEAD_DIM].astype(BF16)
        o_ref[:, cols] = out[:, HEAD_DIM:]

    @pl.when(step == pl.num_programs(0) - 1)
    def _():
        for h in range(heads):
            x_out[h] = x_ref[h].astype(BF16)


def mix(queries, keys, values, beta_cols):
    tokens, width = queries.shape
    heads = width // HEAD_DIM
    return pl.pallas_call(
        mix_kernel,
        grid=(tokens // SPAN,),
        in_specs=[
            pl.BlockSpec((SPAN, width), lambda c: (c, 0)),
            pl.BlockSpec((2, SPAN, width), lambda c: (0, c, 0)),
            pl.BlockSpec((2, SPAN, width), lambda c: (0, c, 0)),
            pl.BlockSpec((2 * SPAN, heads), lambda c: (c, 0)),
        ],
        out_specs=[
            pl.BlockSpec((SPAN, width), lambda c: (c, 0)),
            pl.BlockSpec((SPAN, width), lambda c: (c, 0)),
            pl.BlockSpec((heads, HEAD_DIM, 2 * HEAD_DIM), lambda c: (0, 0, 0)),
        ],
        out_shape=[
            jax.ShapeDtypeStruct((tokens, width), F32),
            jax.ShapeDtypeStruct((tokens, width), BF16),
            jax.ShapeDtypeStruct((heads, HEAD_DIM, 2 * HEAD_DIM), BF16),
        ],
        scratch_shapes=[pltpu.VMEM((heads, HEAD_DIM, 2 * HEAD_DIM), F32)],
        compiler_params=pltpu.CompilerParams(
            dimension_semantics=("arbitrary",), vmem_limit_bytes=VMEM_LIMIT
        ),
    )(queries, keys, values, beta_cols)


def chain_kernel(peers, x_ref, s_ref):
    heads = x_ref.shape[0] // peers
    for h in range(heads):
        state = jnp.zeros((HEAD_DIM, HEAD_DIM), F32)
        for k in range(peers):
            s_ref[k * heads + h] = state.astype(BF16)
            if k < peers - 1:
                maps = x_ref[k * heads + h]
                turn = maps[:, :HEAD_DIM]
                high, low = split(state)
                state = maps[:, HEAD_DIM:].astype(F32) + dot(
                    jnp.concatenate([turn, turn], axis=1), jnp.concatenate([high, low], axis=0)
                )


def start_state(maps, axis):
    peers, index = lax.axis_size(axis), lax.axis_index(axis)
    heads = maps.shape[0]
    spread = heads % peers == 0
    if spread:
        held = lax.all_to_all(maps, axis, split_axis=0, concat_axis=0, tiled=True)
    else:
        held = lax.all_gather(maps, axis, axis=0, tiled=True)
    states = pl.pallas_call(
        functools.partial(chain_kernel, peers),
        out_shape=jax.ShapeDtypeStruct((held.shape[0], HEAD_DIM, HEAD_DIM), BF16),
        compiler_params=pltpu.CompilerParams(vmem_limit_bytes=VMEM_LIMIT),
    )(held)
    if spread:
        return lax.all_to_all(states, axis, split_axis=0, concat_axis=0, tiled=True)
    return lax.dynamic_slice_in_dim(states, index * heads, heads, 0)


def out_kernel(o_ref, m_ref, s_ref, g_ref, w_ref, y_ref, mixed_ref):
    @pl.when(pl.program_id(0) == 0)
    def _():
        for h in range(s_ref.shape[0]):
            cols = slice(h * HEAD_DIM, (h + 1) * HEAD_DIM)
            seen = o_ref[:, cols] + dot(m_ref[:, cols], s_ref[h])
            scale = lax.rsqrt(jnp.mean(seen * seen, axis=1, keepdims=True) + 1e-06)
            gate = g_ref[:, cols].astype(F32)
            mixed_ref[:, cols] = (seen * scale * (gate / (1.0 + jnp.exp(-gate)))).astype(BF16)

    y_ref[...] = dot(mixed_ref[...], w_ref[...]).astype(BF16)


def project(local, reach, states, gate, out_weight):
    tokens, width = local.shape
    total = out_weight.shape[1]
    tile = 512
    whole = pl.BlockSpec((tokens, width), lambda n: (0, 0))
    return pl.pallas_call(
        out_kernel,
        grid=(total // tile,),
        in_specs=[
            whole,
            whole,
            pl.BlockSpec(states.shape, lambda n: (0, 0, 0)),
            whole,
            pl.BlockSpec((width, tile), lambda n: (0, n)),
        ],
        out_specs=pl.BlockSpec((tokens, tile), lambda n: (0, n)),
        out_shape=jax.ShapeDtypeStruct((tokens, total), BF16),
        scratch_shapes=[pltpu.VMEM((tokens, width), BF16)],
        compiler_params=pltpu.CompilerParams(
            dimension_semantics=("arbitrary",), vmem_limit_bytes=VMEM_LIMIT
        ),
    )(local, reach, states, gate, out_weight)


def per_device(queries, keys, values, betas, gate, out_weight):
    heads, _, tokens = betas.shape
    beta_cols = betas.transpose(2, 1, 0).reshape(2 * tokens, heads)
    local, reach, maps = mix(queries, keys, values, beta_cols)
    states = start_state(maps, "ctx")
    partial_sum = project(local, reach, states, gate, out_weight)
    return lax.psum_scatter(partial_sum, "head", scatter_dimension=1, tiled=True)


def solution(mesh):
    return jax.shard_map(
        per_device,
        mesh=mesh,
        in_specs=(
            P("ctx", "head"),
            P(None, "ctx", "head"),
            P(None, "ctx", "head"),
            P("head", None, "ctx"),
            P("ctx", "head"),
            P("head", None),
        ),
        out_specs=P("ctx", "head"),
        check_vma=False,
    )
```

```python
import functools

import jax
import jax.numpy as jnp
from jax import lax
from jax.experimental import pallas as pl
from jax.experimental.pallas import tpu as pltpu
from jax.sharding import PartitionSpec as P

HEAD_DIM = 128
SPAN = 64
BASE = 16
F32 = jnp.float32
BF16 = jnp.bfloat16
VMEM_LIMIT = 60 * 1024 * 1024
MESH = pl.DeviceIdType.MESH
PIECES = 4


def iota(shape, dim):
    return lax.broadcasted_iota(jnp.int32, shape, dim)


def split(a):
    high = a.astype(BF16)
    return high, (a - high.astype(F32)).astype(BF16)


def dot(a, b):
    return jnp.dot(a, b, preferred_element_type=F32)


def dot3(a, b):
    ah, al = split(a)
    bh, bl = split(b)
    return dot(jnp.concatenate([ah, al, ah], axis=1), jnp.concatenate([bh, bh, bl], axis=0))


def inverse(lowers, order):
    lane = iota((BASE, order), 1)
    compact = []
    for low in lowers:
        total = jnp.zeros((BASE, order), F32)
        for blk in range(order // BASE):
            total = jnp.where(lane // BASE == blk, low[blk * BASE : (blk + 1) * BASE, :], total)
        compact.append(total)
    inv = [(iota((BASE, order), 0) == lane % BASE).astype(F32) for _ in lowers]
    for j in range(BASE - 1):
        pick = (lane // BASE) * BASE + j
        for n, low in enumerate(compact):
            column = jnp.take_along_axis(low, pick, axis=1, mode="promise_in_bounds")
            inv[n] = inv[n] - column * inv[n][j : j + 1, :]
    row = iota((order, order), 0)
    col = iota((order, order), 1)
    width = BASE
    while width < order:
        corner = (row // (2 * width) == col // (2 * width)) & (row // width != col // width)
        diagonal = row // width == col // width
        second = (iota((width, order), 1) // width) % 2 == 1
        half = [dot3(jnp.where(second, t, 0.0), jnp.where(corner, low, 0.0)) for t, low in zip(inv, lowers)]
        full = [
            jnp.where(diagonal, jnp.concatenate([t] * (order // width), axis=0), 0.0) for t in inv
        ]
        fill = [dot3(y, e) for y, e in zip(half, full)]
        inv = [
            jnp.concatenate([jnp.where(second, 0.0, t), jnp.where(second, t, 0.0) - r], axis=0)
            for t, r in zip(inv, fill)
        ]
        width *= 2
    return inv


def mix_kernel(q_ref, k_ref, v_ref, b_ref, o_ref, m_ref, x_out, x_ref):
    heads = q_ref.shape[1] // HEAD_DIM
    span = q_ref.shape[0]
    order = 2 * span
    step = pl.program_id(0)

    @pl.when(step == 0)
    def _():
        start = (iota((HEAD_DIM, 2 * HEAD_DIM), 0) == iota((HEAD_DIM, 2 * HEAD_DIM), 1)).astype(F32)
        for h in range(heads):
            x_ref[h] = start

    row = iota((order, order), 0)
    col = iota((order, order), 1)
    strict = col < row
    weave = (row == 2 * (col % span) + col // span).astype(BF16)
    causal = iota((span, order), 1) <= 2 * iota((span, order), 0) + 1
    data = []
    lowers = []
    for h in range(heads):
        cols = slice(h * HEAD_DIM, (h + 1) * HEAD_DIM)
        query = q_ref[:, cols]
        pair = jnp.concatenate(
            [
                jnp.concatenate([k_ref[0, :, cols], v_ref[0, :, cols]], axis=1),
                jnp.concatenate([k_ref[1, :, cols], v_ref[1, :, cols]], axis=1),
            ],
            axis=0,
        )
        woven = dot(weave, pair)
        key = woven[:, :HEAD_DIM]
        value = woven[:, HEAD_DIM:]
        key_b = key.astype(BF16)
        norm = lax.rsqrt(jnp.sum(key * key, axis=1, keepdims=True) + 1e-06)
        beta = b_ref[:, h : h + 1]
        both = jnp.concatenate([key_b, query], axis=0)
        gram = lax.dot_general(both, key_b, (((1,), (1,)), ((), ())), preferred_element_type=F32)
        weight = beta * norm * norm
        lowers.append(jnp.where(strict, weight * gram[:order], 0.0))
        scores = jnp.where(causal, gram[order:], 0.0).astype(BF16)
        qf = query.astype(F32)
        q_norm = lax.rsqrt(jnp.sum(qf * qf, axis=1, keepdims=True) + 1e-06)
        readers = jnp.concatenate([key.T.astype(BF16), scores], axis=0)
        data.append((both, readers, beta * norm * value, weight, q_norm))
    solved = inverse(lowers, order)
    seen = []
    for h in range(heads):
        both = data[h][0]
        high, low = split(x_ref[h])
        seen.append(
            dot(jnp.concatenate([both, both], axis=1), jnp.concatenate([high, low], axis=0))
        )
    writes = []
    for h in range(heads):
        _, _, scaled, weight, _ = data[h]
        gap = -weight * seen[h][:order]
        gap = jnp.concatenate([gap[:, :HEAD_DIM], gap[:, HEAD_DIM:] + scaled], axis=1)
        writes.append(dot3(solved[h], gap))
    for h in range(heads):
        cols = slice(h * HEAD_DIM, (h + 1) * HEAD_DIM)
        readers, q_norm = data[h][1], data[h][4]
        high, low = split(writes[h])
        change = dot(
            jnp.concatenate([readers, readers], axis=1), jnp.concatenate([high, low], axis=0)
        )
        x_ref[h] = x_ref[h] + change[:HEAD_DIM]
        out = q_norm * (seen[h][order:] + change[HEAD_DIM:])
        m_ref[:, cols] = out[:, :HEAD_DIM].astype(BF16)
        o_ref[:, cols] = out[:, HEAD_DIM:]

    @pl.when(step == pl.num_programs(0) - 1)
    def _():
        for h in range(heads):
            x_out[h] = x_ref[h].astype(BF16)


def mix(queries, keys, values, beta_cols):
    tokens, width = queries.shape
    heads = width // HEAD_DIM
    return pl.pallas_call(
        mix_kernel,
        grid=(tokens // SPAN,),
        in_specs=[
            pl.BlockSpec((SPAN, width), lambda c: (c, 0)),
            pl.BlockSpec((2, SPAN, width), lambda c: (0, c, 0)),
            pl.BlockSpec((2, SPAN, width), lambda c: (0, c, 0)),
            pl.BlockSpec((2 * SPAN, heads), lambda c: (c, 0)),
        ],
        out_specs=[
            pl.BlockSpec((SPAN, width), lambda c: (c, 0)),
            pl.BlockSpec((SPAN, width), lambda c: (c, 0)),
            pl.BlockSpec((heads, HEAD_DIM, 2 * HEAD_DIM), lambda c: (0, 0, 0)),
        ],
        out_shape=[
            jax.ShapeDtypeStruct((tokens, width), F32),
            jax.ShapeDtypeStruct((tokens, width), BF16),
            jax.ShapeDtypeStruct((heads, HEAD_DIM, 2 * HEAD_DIM), BF16),
        ],
        scratch_shapes=[pltpu.VMEM((heads, HEAD_DIM, 2 * HEAD_DIM), F32)],
        compiler_params=pltpu.CompilerParams(
            dimension_semantics=("arbitrary",), vmem_limit_bytes=VMEM_LIMIT
        ),
    )(queries, keys, values, beta_cols)


def chain_kernel(peers, x_ref, s_ref):
    heads = x_ref.shape[0] // peers
    for h in range(heads):
        state = jnp.zeros((HEAD_DIM, HEAD_DIM), F32)
        for k in range(peers):
            s_ref[k * heads + h] = state.astype(BF16)
            if k < peers - 1:
                maps = x_ref[k * heads + h]
                turn = maps[:, :HEAD_DIM]
                high, low = split(state)
                state = maps[:, HEAD_DIM:].astype(F32) + dot(
                    jnp.concatenate([turn, turn], axis=1), jnp.concatenate([high, low], axis=0)
                )


def exchange_kernel(axis, peers, maps_ref, own_ref, held, states, out_send, out_recv, back_send, back_recv):
    me = lax.axis_index(axis)
    heads = maps_ref.shape[0] // peers
    barrier = pltpu.get_barrier_semaphore()
    for away in range(1, peers):
        pl.semaphore_signal(
            barrier, inc=1, device_id={axis: lax.rem(me + away, peers)}, device_id_type=MESH
        )
    pl.semaphore_wait(barrier, peers - 1)

    def outward(away):
        peer = lax.rem(me + away, peers)
        return pltpu.make_async_remote_copy(
            src_ref=maps_ref.at[pl.ds(peer * heads, heads)],
            dst_ref=held.at[pl.ds(me * heads, heads)],
            send_sem=out_send.at[away],
            recv_sem=out_recv.at[away],
            device_id={axis: peer},
            device_id_type=MESH,
        )

    def homeward(away):
        peer = lax.rem(me + away, peers)
        return pltpu.make_async_remote_copy(
            src_ref=states.at[pl.ds(peer * heads, heads)],
            dst_ref=own_ref.at[pl.ds(me * heads, heads)],
            send_sem=back_send.at[away],
            recv_sem=back_recv.at[away],
            device_id={axis: peer},
            device_id_type=MESH,
        )

    for away in range(1, peers):
        outward(away).start()
    for h in range(heads):
        held[me * heads + h] = maps_ref[me * heads + h]
    for away in range(1, peers):
        outward(away).wait()
    chain_kernel(peers, held, states)
    for away in range(1, peers):
        homeward(away).start()
    for h in range(heads):
        own_ref[me * heads + h] = states[me * heads + h]
    for away in range(1, peers):
        homeward(away).wait()


def start_state(maps, axis):
    peers, index = lax.axis_size(axis), lax.axis_index(axis)
    heads = maps.shape[0]
    shape = (heads, HEAD_DIM, HEAD_DIM)
    vmem = pl.BlockSpec(memory_space=pltpu.VMEM)
    if heads % peers == 0:
        return pl.pallas_call(
            functools.partial(exchange_kernel, axis, peers),
            in_specs=[vmem],
            out_specs=vmem,
            out_shape=jax.ShapeDtypeStruct(shape, BF16),
            scratch_shapes=[
                pltpu.VMEM(maps.shape, BF16),
                pltpu.VMEM(shape, BF16),
                pltpu.SemaphoreType.DMA((peers,)),
                pltpu.SemaphoreType.DMA((peers,)),
                pltpu.SemaphoreType.DMA((peers,)),
                pltpu.SemaphoreType.DMA((peers,)),
            ],
            compiler_params=pltpu.CompilerParams(
                collective_id=0, has_side_effects=True, vmem_limit_bytes=VMEM_LIMIT
            ),
        )(maps)
    held = lax.all_gather(maps, axis, axis=0, tiled=True)
    states = pl.pallas_call(
        functools.partial(chain_kernel, peers),
        out_shape=jax.ShapeDtypeStruct((held.shape[0], HEAD_DIM, HEAD_DIM), BF16),
        compiler_params=pltpu.CompilerParams(vmem_limit_bytes=VMEM_LIMIT),
    )(held)
    return lax.dynamic_slice_in_dim(states, index * heads, heads, 0)


def reduce_kernel(
    axis, o_ref, m_ref, s_ref, g_ref, w_ref, y_ref,
    mixed, weight, total, far_out, far_in, near_out, near_in, cross_out, cross_in,
    load_sem, far_send, far_recv, near_send, near_recv, cross_send, cross_recv,
):
    me = lax.axis_index(axis)
    chip, core = me // 2, me % 2
    sibling = 2 * chip + 1 - core
    across = 2 * (1 - chip) + core
    beyond = 2 * (1 - chip) + 1 - core
    width = y_ref.shape[1]
    rows = y_ref.shape[0] // PIECES

    loads = []
    for n, owner in enumerate((beyond, across, sibling, me)):
        loads.append(
            pltpu.make_async_copy(
                w_ref.at[:, pl.ds(pl.multiple_of(owner * width, width), width)],
                weight.at[n],
                load_sem.at[n],
            )
        )
        loads[n].start()

    barrier = pltpu.get_barrier_semaphore()
    for other in (sibling, across):
        pl.semaphore_signal(barrier, inc=1, device_id={axis: other}, device_id_type=MESH)
    pl.semaphore_wait(barrier, 2)

    def send(source, target, send_sem, recv_sem, t, device):
        return pltpu.make_async_remote_copy(
            src_ref=source.at[t],
            dst_ref=target.at[t],
            send_sem=send_sem.at[t],
            recv_sem=recv_sem.at[t],
            device_id={axis: device},
            device_id_type=MESH,
        )

    def far(t):
        return send(far_out, far_in, far_send, far_recv, t, sibling)

    def near(t):
        return send(near_out, near_in, near_send, near_recv, t, sibling)

    def cross(t):
        return send(cross_out, cross_in, cross_send, cross_recv, t, across)

    def pass_on(t):
        far(t).wait()
        cross_out[t] = (total[t] + far_in[t].astype(F32)).astype(BF16)
        cross(t).start()

    for t in range(PIECES):
        span = slice(t * rows, (t + 1) * rows)
        for h in range(s_ref.shape[0]):
            cols = slice(h * HEAD_DIM, (h + 1) * HEAD_DIM)
            seen = o_ref[span, cols] + dot(m_ref[span, cols], s_ref[h])
            scale = lax.rsqrt(jnp.mean(seen * seen, axis=1, keepdims=True) + 1e-06)
            gate = g_ref[span, cols].astype(F32)
            mixed[t, :, cols] = (seen * scale * (gate / (1.0 + jnp.exp(-gate)))).astype(BF16)
        if t == 0:
            loads[0].wait()
        far_out[t] = dot(mixed[t], weight[0]).astype(BF16)
        far(t).start()
        if t == 0:
            loads[1].wait()
        total[t] = dot(mixed[t], weight[1])
        if t > 0:
            pass_on(t - 1)
    loads[2].wait()
    for t in range(PIECES):
        near_out[t] = dot(mixed[t], weight[2]).astype(BF16)
        near(t).start()
        if t == 0:
            pass_on(PIECES - 1)
    loads[3].wait()
    for t in range(PIECES):
        total[t] = dot(mixed[t], weight[3])
    for t in range(PIECES):
        near(t).wait()
        cross(t).wait()
        y_ref[t * rows : (t + 1) * rows, :] = (
            total[t] + near_in[t].astype(F32) + cross_in[t].astype(F32)
        ).astype(BF16)


def project_reduce(local, reach, states, gate, out_weight, axis):
    tokens, depth = local.shape
    width = out_weight.shape[1] // lax.axis_size(axis)
    vmem = pl.BlockSpec(memory_space=pltpu.VMEM)
    piece = (PIECES, tokens // PIECES, width)
    return pl.pallas_call(
        functools.partial(reduce_kernel, axis),
        in_specs=[vmem, vmem, vmem, vmem, pl.BlockSpec(memory_space=pl.ANY)],
        out_specs=vmem,
        out_shape=jax.ShapeDtypeStruct((tokens, width), BF16),
        scratch_shapes=[
            pltpu.VMEM((PIECES, tokens // PIECES, depth), BF16),
            pltpu.VMEM((4, depth, width), BF16),
            pltpu.VMEM(piece, F32),
        ]
        + [pltpu.VMEM(piece, BF16)] * 6
        + [pltpu.SemaphoreType.DMA((4,))]
        + [pltpu.SemaphoreType.DMA((PIECES,))] * 6,
        compiler_params=pltpu.CompilerParams(
            collective_id=1, has_side_effects=True, vmem_limit_bytes=VMEM_LIMIT
        ),
    )(local, reach, states, gate, out_weight)


def out_kernel(o_ref, m_ref, s_ref, g_ref, w_ref, y_ref, mixed_ref):
    @pl.when(pl.program_id(0) == 0)
    def _():
        for h in range(s_ref.shape[0]):
            cols = slice(h * HEAD_DIM, (h + 1) * HEAD_DIM)
            seen = o_ref[:, cols] + dot(m_ref[:, cols], s_ref[h])
            scale = lax.rsqrt(jnp.mean(seen * seen, axis=1, keepdims=True) + 1e-06)
            gate = g_ref[:, cols].astype(F32)
            mixed_ref[:, cols] = (seen * scale * (gate / (1.0 + jnp.exp(-gate)))).astype(BF16)

    y_ref[...] = dot(mixed_ref[...], w_ref[...]).astype(BF16)


def project(local, reach, states, gate, out_weight):
    tokens, width = local.shape
    total = out_weight.shape[1]
    tile = 512
    whole = pl.BlockSpec((tokens, width), lambda n: (0, 0))
    return pl.pallas_call(
        out_kernel,
        grid=(total // tile,),
        in_specs=[
            whole,
            whole,
            pl.BlockSpec(states.shape, lambda n: (0, 0, 0)),
            whole,
            pl.BlockSpec((width, tile), lambda n: (0, n)),
        ],
        out_specs=pl.BlockSpec((tokens, tile), lambda n: (0, n)),
        out_shape=jax.ShapeDtypeStruct((tokens, total), BF16),
        scratch_shapes=[pltpu.VMEM((tokens, width), BF16)],
        compiler_params=pltpu.CompilerParams(
            dimension_semantics=("arbitrary",), vmem_limit_bytes=VMEM_LIMIT
        ),
    )(local, reach, states, gate, out_weight)


def per_device(queries, keys, values, betas, gate, out_weight):
    heads, _, tokens = betas.shape
    beta_cols = betas.transpose(2, 1, 0).reshape(2 * tokens, heads)
    local, reach, maps = mix(queries, keys, values, beta_cols)
    states = start_state(maps, "ctx")
    if lax.axis_size("head") == 4:
        return project_reduce(local, reach, states, gate, out_weight, "head")
    partial_sum = project(local, reach, states, gate, out_weight)
    return lax.psum_scatter(partial_sum, "head", scatter_dimension=1, tiled=True)


def solution(mesh):
    return jax.shard_map(
        per_device,
        mesh=mesh,
        in_specs=(
            P("ctx", "head"),
            P(None, "ctx", "head"),
            P(None, "ctx", "head"),
            P("head", None, "ctx"),
            P("ctx", "head"),
            P("head", None),
        ),
        out_specs=P("ctx", "head"),
        check_vma=False,
    )
```
